128 devices in a mesh: prow: 8 (over z_hi, y), pcol: 16 (over x, z_lo, core).
Axes of the slice: x: 4, y: 4, z: 4 (z_hi: 2, z_lo: 2; z = z_hi * 2 + z_lo), core: 2. Of those that a mesh axis runs over, the one named last changes fastest.
Arguments:
- panel_t: float32 [16, 256, 8192], P('pcol', None, 'prow'), may hold values from -0.0625 to 0.0625
- ancestor: float32 [8192, 8192], P('prow', 'pcol'), as said below
- structure: int32 [16, 32], replicated, may hold values 0 or 1
- diag_inv: float32 [16, 256, 256], P('pcol'), may hold values from -6 to 6
Outputs:
- inverse_panel: float32 [4096, 8192], P('pcol', 'prow')
- inverse_diag: float32 [16, 256, 256], P('pcol')
The draws below stay inside these ranges and needn't reach their ends.
Inputs may be any that keep to these rules, and one draw needn't show every extreme that they name: ancestor is symmetric up to rounding.
All inputs are finite; a program needn't handle non-finite values.
Results may differ from the reference program's by a relative error of at most 0.00007.
Values sent between devices are 32-bit elements; how exact they have to be, the bound alone decides.
No kernel may reach another device: no remote copies, remote signals or barrier semaphores. Data moves between devices by JAX's collectives and lax.ppermute only.
A program may use at most 128 MiB of HBM per device.

```python
import jax
import jax.numpy as jnp
from jax import lax

B = 256
S = 16
NA = 32
R = 8192


def draw_ancestor(key, part):
    first = jax.random.normal(jax.random.fold_in(key, 11), (R, R), jnp.float32)
    matrix = (first + first.T) * 0.7071
    return matrix


def place_ends(array, key, smallest, high):
    longest = array.shape.index(max(array.shape))
    spots = []
    for shift in (0, 1):
        where = [jax.random.randint(jax.random.fold_in(key, axis), (), 0, length) for axis, length in enumerate(array.shape)]
        where[longest] = (where[longest] + shift) % array.shape[longest]
        spots.append(tuple(where))
    return array.at[spots[0]].set(smallest).at[spots[1]].set(high)


def level_of(own_key, dims, split, smallest, top_value):
    def one(axis_at, parts):
        steps = jax.random.uniform(jax.random.fold_in(jax.random.fold_in(own_key, 6), axis_at), (parts,), jnp.float32, smallest / len(split), top_value / len(split))
        return jnp.repeat(jnp.exp(steps), dims[axis_at] // parts).reshape((-1,) + (1,) * (len(dims) - axis_at - 1))

    factor_of = one(*split[0])
    for cut in split[1:]:
        factor_of = factor_of * one(*cut)
    return factor_of


def gaussian(own_key, extent, spread, reach, split=(), held_as=jnp.bfloat16):
    values = jax.random.normal(own_key, extent, jnp.float32) * spread
    if len(split) > 0:
        values = level_of(own_key, extent, split, -0.22, 0.18) * values
    return jnp.clip(values, min=-reach, max=reach).astype(held_as)


def setup_inputs(seed: int = 0) -> dict:
    key_of = jax.random.split(jax.random.key(seed), 5)
    panel_t = gaussian(key_of[0], (S, B, R), R ** -0.5, 0.0625, ((0, 16), (2, 8)), jnp.float32)
    ancestor = draw_ancestor(jax.random.fold_in(key_of[4], 71), 0)
    structure = place_ends((jax.random.randint(key_of[2], (S, NA), 0, 4) < 3).astype(jnp.int32), jax.random.fold_in(key_of[2], 1), 0, 1)
    diag_inv = gaussian(key_of[3], (S, B, B), 1.0, 6.0, ((0, 16),), jnp.float32)
    return dict(panel_t=panel_t, ancestor=ancestor, structure=structure, diag_inv=diag_inv)


def reference(panel_t, ancestor, structure, diag_inv):
    mask = jnp.repeat(structure.astype(jnp.float32), B, axis=1)
    masked = panel_t * mask[:, None, :]
    flat = masked.reshape(S * B, R)
    inverse_panel = -jnp.dot(flat, ancestor, precision=lax.Precision.HIGHEST, preferred_element_type=jnp.float32)
    blocks = inverse_panel.reshape(S, B, R)
    inverse_diag = diag_inv - jnp.einsum("kbj,kcj->kbc", blocks, masked, precision=lax.Precision.HIGHEST)
    return inverse_panel, inverse_diag
```

```python
import jax
import jax.numpy as jnp
from jax import lax
from jax.sharding import PartitionSpec as P

AXES = ("prow", "pcol")
CHUNKS = 4


def number(x, y, z, core):
    return ((z >> 1) * 4 + y) * 16 + x * 4 + (z & 1) * 2 + core


def pairs(move, keep=lambda x, y, z: True):
    found = []
    for x in range(4):
        for y in range(4):
            for z in range(4):
                if keep(x, y, z):
                    for core in range(2):
                        tx, ty, tz, tc = move(x, y, z, core)
                        found.append((number(x, y, z, core), number(tx % 4, ty % 4, tz % 4, tc)))
    return found


def is_on(x, y, z):
    return (y & 1) == (z & 1)


def is_off(x, y, z):
    return (y & 1) != (z & 1)


X_UP = pairs(lambda x, y, z, c: (x + 1, y, z, c))
X_DOWN = pairs(lambda x, y, z, c: (x - 1, y, z, c))
CORE = pairs(lambda x, y, z, c: (x, y, z, 1 - c))
Z_MATE = pairs(lambda x, y, z, c: (x, y, z ^ 1, c))
OFF_Z_UP = pairs(lambda x, y, z, c: (x, y, z + 1, c), is_off)
OFF_Z_DOWN = pairs(lambda x, y, z, c: (x, y, z - 1, c), is_off)
ON_Z_FAR = pairs(lambda x, y, z, c: (x, y, z + 2, c), is_on)
ON_Y_UP = pairs(lambda x, y, z, c: (x, y + 1, z, c), is_on)
ON_Y_DOWN = pairs(lambda x, y, z, c: (x, y - 1, z, c), is_on)
OFF_Y_UP = pairs(lambda x, y, z, c: (x, y + 1, z, c), is_off)
OFF_Y_DOWN = pairs(lambda x, y, z, c: (x, y - 1, z, c), is_off)


def send(array, route):
    return lax.ppermute(array, AXES, route)


def product(left, right):
    return lax.dot_general(
        left,
        right,
        (((1,), (1,)), ((), ())),
        precision=lax.Precision.HIGH,
        preferred_element_type=jnp.float32,
    )


def local(panel_t, ancestor, structure, diag_inv):
    width = panel_t.shape[1]
    span = panel_t.shape[2]
    half = span // 2
    row_blocks = span // width
    prow = lax.axis_index("prow")
    pcol = lax.axis_index("pcol")
    x = pcol // 4
    y = prow % 4
    z_high = prow // 4
    z_low = (pcol // 2) % 2
    z = z_high * 2 + z_low
    core = pcol % 2
    mine = lax.dynamic_slice(structure, (pcol, prow * row_blocks), (1, row_blocks))
    masked = panel_t.reshape(width, row_blocks, width) * mine.astype(jnp.float32).reshape(1, row_blocks, 1)
    masked = masked.reshape(width, span)
    own = jnp.where(core == 0, masked, jnp.concatenate([masked[:, half:], masked[:, :half]], axis=1))

    below = send(own, OFF_Z_UP)
    above = send(own, OFF_Z_DOWN)
    far = send(own, ON_Z_FAR)
    on = (y & 1) == (z & 1)

    def columns(item):
        left = send(item, ON_Y_UP)
        right = send(item, ON_Y_DOWN)
        top = send(left[: width // 2], OFF_Y_UP)
        bottom = send(right[width // 2 :], OFF_Y_DOWN)
        first = jnp.where(on, item, left)
        second = jnp.where(on, jnp.concatenate([top, bottom], axis=0), right)
        return first, second

    first_y = jnp.where(on, y, (y + 3) % 4)
    same_first = (first_y >> 1) == (x & 1)
    left_high = ((x + 3) % 4) >> 1

    def in_order(item_a, high_a, item_b):
        a_first, a_second = columns(item_a)
        b_first, b_second = columns(item_b)
        a_same = jnp.where(same_first, a_first, a_second)
        a_other = jnp.where(same_first, a_second, a_first)
        b_same = jnp.where(same_first, b_first, b_second)
        b_other = jnp.where(same_first, b_second, b_first)
        own_is_a = high_a == (x >> 1)
        left_is_a = high_a == left_high
        return (
            jnp.where(own_is_a, a_same, b_same),
            jnp.where(left_is_a, a_other, b_other),
            jnp.where(left_is_a, b_other, a_other),
            jnp.where(own_is_a, b_same, a_same),
        )

    mate_rows = in_order(below, ((z + 3) % 4) >> 1, above)
    own_rows = in_order(own, z_high, far)

    step = ancestor.shape[0] // CHUNKS
    out = []
    for q in range(CHUNKS):
        piece = ancestor[q * step : (q + 1) * step]
        left = send(piece, X_UP)
        right = send(piece, X_DOWN)
        top = send(left[: step // 2], X_UP)
        bottom = send(right[step // 2 :], X_DOWN)
        here = [piece, left, right, jnp.concatenate([top, bottom], axis=0)]
        there = [send(part, CORE) for part in here]

        def total(rows):
            acc = None
            for item, a, b in zip(rows, here, there):
                both = product(item[:, :half], a) + product(item[:, half:], b)
                acc = both if acc is None else acc + both
            return acc

        other = send(total(mate_rows), Z_MATE)
        out.append(-(total(own_rows) + other))
    inverse_panel = jnp.concatenate(out, axis=1)

    partial = product(inverse_panel, masked)
    prow_size = lax.axis_size("prow")
    pieces = lax.all_to_all(
        partial.reshape(prow_size, width // prow_size, width), "prow", 0, 0, tiled=True
    )
    summed = lax.all_gather(jnp.sum(pieces, axis=0), "prow", axis=0, tiled=True)
    return inverse_panel, diag_inv - summed[None]


def solution(mesh):
    return jax.shard_map(
        local,
        mesh=mesh,
        in_specs=(P("pcol", None, "prow"), P("prow", "pcol"), P(), P("pcol", None, None)),
        out_specs=(P("pcol", "prow"), P("pcol", None, None)),
        check_vma=False,
    )
```

```python
import jax
import jax.numpy as jnp
from jax import lax
from jax.experimental import pallas as pl
from jax.experimental.pallas import tpu as pltpu
from jax.sharding import PartitionSpec as P


AXES = ("prow", "pcol")
TILE = 256


def number(x, y, z, core):
    return ((z >> 1) * 4 + y) * 16 + x * 4 + (z & 1) * 2 + core


def pairs(on=None, off=None):
    found = []
    for x in range(4):
        for y in range(4):
            for z in range(4):
                move = on if (y & 1) == (z & 1) else off
                if move is not None:
                    for core in range(2):
                        tx, ty, tz, tc = move(x, y, z, core)
                        found.append((number(x, y, z, core), number(tx % 4, ty % 4, tz % 4, tc)))
    return found


def shift(dy, dz):
    return lambda x, y, z, c: (x, y + dy, z + dz, c)


def both(move):
    return pairs(move, move)


X_UP = both(lambda x, y, z, c: (x + 1, y, z, c))
X_DOWN = both(lambda x, y, z, c: (x - 1, y, z, c))
CORE = both(lambda x, y, z, c: (x, y, z, 1 - c))
Z_MATE = both(lambda x, y, z, c: (x, y, z ^ 1, c))
Z_FAR = both(shift(0, 2))
Y_BY = [None] + [both(shift(d, 0)) for d in (1, 2, 3)]
P_ROUTES = [
    pairs(off=shift(0, 1), on=shift(1, 0)),
    pairs(off=shift(0, -1), on=shift(1, 2)),
    pairs(off=shift(2, 1), on=shift(-1, 0)),
    pairs(off=shift(2, -1), on=shift(-1, 2)),
]
Q_ROUTES = [
    pairs(off=shift(1, 1)),
    pairs(off=shift(1, -1), on=shift(0, 2)),
    pairs(off=shift(-1, 1), on=shift(2, 0)),
    pairs(off=shift(-1, -1), on=shift(2, 2)),
]
TO_OFF_MATE = pairs(on=lambda x, y, z, c: (x, y, z ^ 1, c))


def send(array, route):
    return lax.ppermute(array, AXES, route)


def parts(value):
    high = value.astype(jnp.bfloat16)
    return high, (value - high.astype(jnp.float32)).astype(jnp.bfloat16)


def dot(a, b):
    return lax.dot_general(a, b, (((1,), (1,)), ((), ())), preferred_element_type=jnp.float32)


def multiply_kernel(place, x0, x1, x2, x3, *rest):
    pieces = rest[:8]
    out, high, low = rest[8:]
    half = x0.shape[1] // 2

    @pl.when(pl.program_id(0) == 0)
    def _():
        for slot, ref in enumerate((x0, x1, x2, x3)):
            for g in range(2):
                a, b = parts(ref[:, g * half : (g + 1) * half])
                at = place[slot] * 2 + (g ^ place[4])
                high[at] = a
                low[at] = b

    acc = jnp.zeros(out.shape, jnp.float32)
    for j in range(8):
        a, b = parts(pieces[j][...])
        acc += dot(high[j], a) + dot(high[j], b) + dot(low[j], a)
    out[...] = acc


def multiply(place, slots, pieces):
    rows, span = slots[0].shape
    half = span // 2
    count = pieces[0].shape[0]
    whole = pl.BlockSpec((rows, span), lambda i, place: (0, 0))
    tile = pl.BlockSpec((TILE, half), lambda i, place: (i, 0))
    return pl.pallas_call(
        multiply_kernel,
        grid_spec=pltpu.PrefetchScalarGridSpec(
            num_scalar_prefetch=1,
            grid=(count // TILE,),
            in_specs=[whole] * 4 + [tile] * 8,
            out_specs=pl.BlockSpec((rows, TILE), lambda i, place: (0, i)),
            scratch_shapes=[pltpu.VMEM((8, rows, half), jnp.bfloat16)] * 2,
        ),
        out_shape=jax.ShapeDtypeStruct((rows, count), jnp.float32),
        compiler_params=pltpu.CompilerParams(vmem_limit_bytes=40 * 2**20),
        cost_estimate=pl.CostEstimate(
            flops=6 * rows * span * 4 * count, bytes_accessed=4 * (rows * span * 5 + span * 4 * count), transcendentals=0
        ),
    )(place, *slots, *pieces)


def product(left, right):
    return lax.dot_general(
        left,
        right,
        (((1,), (1,)), ((), ())),
        precision=lax.Precision.HIGH,
        preferred_element_type=jnp.float32,
    )


def local(panel_t, ancestor, structure, diag_inv):
    width = panel_t.shape[1]
    span = panel_t.shape[2]
    row_blocks = span // width
    prow = lax.axis_index("prow")
    pcol = lax.axis_index("pcol")
    x = pcol // 4
    y = prow & 3
    z = (prow >> 2) * 2 + ((pcol >> 1) & 1)
    core = pcol & 1
    on = (y & 1) == (z & 1)
    mine = lax.dynamic_slice(structure, (pcol, prow * row_blocks), (1, row_blocks))
    masked = panel_t.reshape(width, row_blocks, width) * mine.astype(jnp.float32).reshape(1, row_blocks, 1)
    own = masked.reshape(width, span)

    half = ancestor.shape[0] // 2
    left = send(ancestor, X_UP)
    right = send(ancestor, X_DOWN)
    p_slots = [send(own, route) for route in P_ROUTES]
    q_slots = [send(own, route) for route in Q_ROUTES]
    to_off = send(own, TO_OFF_MATE)
    far = jnp.concatenate([send(left[:half], X_UP), send(right[half:], X_DOWN)], axis=0)
    here = [ancestor, left, right, far]
    there = [send(piece, CORE) for piece in here]
    pieces = [piece for pair in zip(here, there) for piece in pair]

    first_y = jnp.where(on, y, (y + 3) & 3)
    p_high = jnp.where(on, ((z + 3) & 3) >> 1, z >> 1)
    q_high = jnp.where(on, z >> 1, ((z + 3) & 3) >> 1)

    def places(high):
        found = []
        for a in range(2):
            for r in range(2):
                block = (high ^ r) * 2 + ((first_y >> 1) ^ a)
                delta = (block - x) & 3
                found.append(jnp.where(delta == 0, 0, jnp.where(delta == 3, 1, delta + 1)))
        return jnp.stack(found + [core] + [core] * 3).astype(jnp.int32)

    q_slots[0] = jnp.where(on, own, q_slots[0])
    p_out = multiply(places(p_high), p_slots, pieces)
    q_out = multiply(places(q_high), q_slots, pieces)
    mate_out = jnp.where(on, p_out, q_out)
    own_out = jnp.where(on, q_out, p_out)

    mate_panel = jnp.where(on, jnp.where((z & 1) == 1, p_slots[0], p_slots[1]), to_off)
    mate_diag = send(product(mate_out, mate_panel), Z_MATE)
    inverse_panel = -(own_out + send(mate_out, Z_MATE))
    partial = product(own_out, own) + mate_diag

    quarter = width // 4
    cut = partial.reshape(4, quarter, width)
    summed = lax.dynamic_index_in_dim(cut, y, 0, False)
    for d in (1, 2, 3):
        summed = summed + send(lax.dynamic_index_in_dim(cut, (y + d) & 3, 0, False), Y_BY[d])
    summed = summed + send(summed, Z_FAR)
    diag = jnp.zeros((4, quarter, width), jnp.float32)
    diag = lax.dynamic_update_index_in_dim(diag, summed, y, 0)
    for d in (1, 2, 3):
        diag = lax.dynamic_update_index_in_dim(diag, send(summed, Y_BY[d]), (y - d) & 3, 0)
    return inverse_panel, diag_inv + diag.reshape(1, width, width)


def solution(mesh):
    return jax.shard_map(
        local,
        mesh=mesh,
        in_specs=(P("pcol", None, "prow"), P("prow", "pcol"), P(), P("pcol", None, None)),
        out_specs=(P("pcol", "prow"), P("pcol", None, None)),
        check_vma=False,
    )
```

```python
import jax
import jax.numpy as jnp
from jax import lax
from jax.experimental import pallas as pl
from jax.experimental.pallas import tpu as pltpu
from jax.sharding import PartitionSpec as P


AXES = ("prow", "pcol")
TILE = 256


def number(x, y, z, core):
    return ((z >> 1) * 4 + y) * 16 + x * 4 + (z & 1) * 2 + core


def pairs(on=None, off=None):
    found = []
    for x in range(4):
        for y in range(4):
            for z in range(4):
                move = on if (y & 1) == (z & 1) else off
                if move is not None:
                    for core in range(2):
                        tx, ty, tz, tc = move(x, y, z, core)
                        found.append((number(x, y, z, core), number(tx % 4, ty % 4, tz % 4, tc)))
    return found


def shift(dy, dz):
    return lambda x, y, z, c: (x, y + dy, z + dz, c)


def both(move):
    return pairs(move, move)


X_UP = both(lambda x, y, z, c: (x + 1, y, z, c))
X_DOWN = both(lambda x, y, z, c: (x - 1, y, z, c))
CORE = both(lambda x, y, z, c: (x, y, z, 1 - c))
Y_BY = [None] + [both(shift(d, 0)) for d in (1, 2, 3)]
Z_FLIP = [None] + [both(lambda x, y, z, c, d=d: (x, y, z ^ d, c)) for d in (1, 2, 3)]


def send(array, route):
    return lax.ppermute(array, AXES, route)


def parts(value):
    high = value.astype(jnp.bfloat16)
    return high, (value - high.astype(jnp.float32)).astype(jnp.bfloat16)


def dot(a, b):
    return lax.dot_general(a, b, (((1,), (1,)), ((), ())), preferred_element_type=jnp.float32)


SLOTS = [
    ((0, -1), (-1, 2)),
    ((0, 1), (1, 2)),
    ((2, -1), (1, -1)),
    ((2, 1), (1, 1)),
    ((0, 0), (-1, 0)),
    ((2, 0), (1, 0)),
    ((0, 2), (-1, -1)),
    ((2, 2), (-1, 1)),
]


def slot_info(where, structure, entry, blocks):
    x, y, z, core = where[0], where[1], where[2], where[3]
    on = (y & 1) == (z & 1)
    ys = (y + jnp.where(on, entry[0][0], entry[1][0])) & 3
    zs = (z + jnp.where(on, entry[0][1], entry[1][1])) & 3
    block = (zs >> 1) * 4 + ys
    delta = ((block >> 1) - x) & 3
    place = jnp.where(delta == 0, 0, jnp.where(delta == 3, 1, delta + 1))
    supernode = x * 4 + (zs & 1) * 2 + core
    return place, [structure[supernode, block * blocks + b].astype(jnp.float32) for b in range(blocks)]


def cut_panel(value, keeps, at, high, low):
    rows = high.shape[2]
    for b, keep in enumerate(keeps):
        hi, lo = parts(value(b) * keep)
        g, inner = divmod(b * rows, high.shape[3])
        high[at, g, :, inner : inner + rows] = hi
        low[at, g, :, inner : inner + rows] = lo


def cut_ancestor(core, pieces, high, low):
    first = pl.program_id(0) < pl.num_programs(0) // 2
    values = [pieces[0][...], pieces[1][...]]
    for at in range(2, len(pieces), 2):
        values.append(jnp.where(first, pieces[at][...], pieces[at + 1][...]))
    for j, value in enumerate(values):
        at = (j // 2) * 2 + (core ^ (j % 2))
        high[at], low[at] = parts(value)


def slot_product(at, place, xh, xl, ah, al):
    acc = None
    for g in range(2):
        a, b = ah[place * 2 + g], al[place * 2 + g]
        term = dot(xh[at, g], a) + dot(xh[at, g], b) + dot(xl[at, g], a)
        acc = term if acc is None else acc + term
    return acc


def early_kernel(where, structure, *refs):
    own, from_left, opposite, from_right, two_off, t0, s0, s1 = refs[:8]
    pieces = refs[8:22]
    own_out, mate_out, xh, xl, ah, al = refs[22:]
    rows, span = own.shape
    blocks = span // rows
    on = (where[1] & 1) == (where[2] & 1)
    infos = [slot_info(where, structure, SLOTS[i], blocks) for i in (0, 1, 4, 5, 6)]

    @pl.when(pl.program_id(0) == 0)
    def _():
        choices = [(s0, s0), (s1, s1), (own, from_left), (opposite, from_right), (two_off, t0)]
        for at, ((a, b), (_, keeps)) in enumerate(zip(choices, infos)):

            def value(i, a=a, b=b):
                part = slice(i * rows, (i + 1) * rows)
                return a[:, part] if a is b else jnp.where(on, a[:, part], b[:, part])

            cut_panel(value, keeps, at, xh, xl)

    cut_ancestor(where[3], pieces, ah, al)
    terms = [slot_product(at, place, xh, xl, ah, al) for at, (place, _) in enumerate(infos)]
    sides = terms[0] + terms[1]
    own_out[...] = terms[2] + terms[3] + jnp.where(on, terms[4], sides)
    mate_out[...] = jnp.where(on, sides, terms[4])


def late_kernel(where, structure, *refs):
    s2, s3, w_top, w_bottom, t1, own_in, mate_in, own, s0, s1 = refs[:10]
    pieces = refs[10:24]
    own_out, mate_out, diag, xh, xl, ah, al = refs[24:]
    rows, span = s2.shape
    blocks = span // rows
    step = pl.program_id(0)
    y, z, core = where[1], where[2], where[3]
    on = (y & 1) == (z & 1)
    infos = [slot_info(where, structure, SLOTS[i], blocks) for i in (2, 3, 7)]

    @pl.when(step == 0)
    def _():
        def last(i):
            part = slice(i * rows, (i + 1) * rows)
            return jnp.where(on, jnp.concatenate([w_top[:, part], w_bottom[:, part]], axis=0), t1[:, part])

        cut_panel(lambda i: s2[:, i * rows : (i + 1) * rows], infos[0][1], 0, xh, xl)
        cut_panel(lambda i: s3[:, i * rows : (i + 1) * rows], infos[1][1], 1, xh, xl)
        cut_panel(last, infos[2][1], 2, xh, xl)
        diag[...] = jnp.zeros(diag.shape, jnp.float32)

    cut_ancestor(core, pieces, ah, al)
    terms = [slot_product(at, place, xh, xl, ah, al) for at, (place, _) in enumerate(infos)]
    own_sum = own_in[...] + jnp.where(on, terms[2], 0.0)
    mate_sum = mate_in[...] + terms[0] + terms[1] + jnp.where(on, 0.0, terms[2])
    own_out[...] = own_sum
    mate_out[...] = mate_sum

    column = ((z >> 1) * 4 + y) * blocks + step
    supernode = where[0] * 4 + (z & 1) * 2 + core
    keep_own = structure[supernode, column].astype(jnp.float32)
    keep_mate = structure[supernode ^ 2, column].astype(jnp.float32)
    panels = (own[...] * keep_own, jnp.where((z & 1) == 1, s0[...], s1[...]) * keep_mate)
    for r, (result, panel) in enumerate(zip((own_sum, mate_sum), panels)):
        a, b = parts(result)
        c, d = parts(panel)
        diag[r] += dot(a, c) + dot(a, d) + dot(b, c)

    @pl.when(step == pl.num_programs(0) - 1)
    def _():
        total = diag[0]
        diag[0] = total + jnp.where(on, 0.0, total.T)
        diag[1] = jnp.where(on, diag[1], 0.0)


def piece_specs(count, half):
    middle = count // TILE // 2
    every = pl.BlockSpec((TILE, half), lambda i, *_: (i, 0))
    top = pl.BlockSpec((TILE, half), lambda i, *_: (jnp.minimum(i, middle - 1), 0))
    bottom = pl.BlockSpec((TILE, half), lambda i, *_: (jnp.maximum(i - middle, 0), 0))
    return [every, every] + [top, bottom] * 6


def run(kernel, where, structure, fixed, tiles, pieces, with_diag):
    rows, span = fixed[0].shape
    half = span // 2
    count = pieces[0].shape[0]
    at_column = pl.BlockSpec((rows, TILE), lambda i, *_: (0, i))
    specs = [pl.BlockSpec(a.shape, lambda i, *_: (0, 0)) for a in fixed] + [at_column] * len(tiles)
    out = jax.ShapeDtypeStruct((rows, count), jnp.float32)
    outs, out_specs = [out, out], [at_column, at_column]
    if with_diag:
        outs.append(jax.ShapeDtypeStruct((2, rows, rows), jnp.float32))
        out_specs.append(pl.BlockSpec((2, rows, rows), lambda i, *_: (0, 0, 0)))
    slots = 3 if with_diag else 5
    return pl.pallas_call(
        kernel,
        grid_spec=pltpu.PrefetchScalarGridSpec(
            num_scalar_prefetch=2,
            grid=(count // TILE,),
            in_specs=specs + piece_specs(count, half),
            out_specs=out_specs,
            scratch_shapes=[pltpu.VMEM((slots, 2, rows, half), jnp.bfloat16)] * 2
            + [pltpu.VMEM((8, TILE, half), jnp.bfloat16)] * 2,
        ),
        out_shape=outs,
        compiler_params=pltpu.CompilerParams(vmem_limit_bytes=56 * 2**20),
        cost_estimate=pl.CostEstimate(
            flops=6 * slots * rows * span * count, bytes_accessed=4 * (rows * span * 10 + span * 4 * count), transcendentals=0
        ),
    )(where, structure, *fixed, *tiles, *pieces)


def local(panel_t, ancestor, structure, diag_inv):
    width = panel_t.shape[1]
    span = panel_t.shape[2]
    prow = lax.axis_index("prow")
    pcol = lax.axis_index("pcol")
    x = pcol >> 2
    y = prow & 3
    z = (prow >> 2) * 2 + ((pcol >> 1) & 1)
    core = pcol & 1
    on = (y & 1) == (z & 1)
    own = panel_t.reshape(width, span)
    split = width // 2
    half = ancestor.shape[0] // 2
    top, bottom = ancestor[:half], ancestor[half:]

    from_left = send(own, both(shift(1, 0)))
    from_right = send(own, both(shift(-1, 0)))
    two_off = send(own, pairs(on=shift(0, 2)))
    opposite = jnp.concatenate(
        [send(from_left[:split], both(shift(1, 0))), send(from_right[split:], both(shift(-1, 0)))],
        axis=0,
    )
    turned = jnp.where(on, two_off, own)
    s0 = send(turned, pairs(on=shift(1, 0), off=shift(0, 1)))
    s1 = send(turned, pairs(on=shift(-1, 0), off=shift(0, -1)))
    t0 = send(from_left, pairs(on=shift(0, 1)))
    t1 = send(from_left, pairs(on=shift(0, -1)))
    crossed = jnp.where(on, from_right, opposite)
    s2 = send(crossed, pairs(on=shift(0, 1), off=shift(0, 1)))
    s3 = send(crossed, pairs(on=shift(0, -1), off=shift(0, -1)))
    w_top = send(s0[:split], pairs(off=shift(1, 0)))
    w_bottom = send(s1[split:], pairs(off=shift(-1, 0)))

    halves = [send(top, X_UP), send(bottom, X_UP), send(top, X_DOWN), send(bottom, X_DOWN)]
    halves += [send(halves[0], X_UP), send(halves[3], X_DOWN)]
    pieces = [ancestor, send(ancestor, CORE)]
    for i in range(0, 6, 2):
        pair = halves[i : i + 2]
        pieces += pair + [send(piece, CORE) for piece in pair]

    where = jnp.stack([x, y, z, core]).astype(jnp.int32)
    own_part, mate_part = run(
        early_kernel, where, structure, [own, from_left, opposite, from_right, two_off, t0, s0, s1], [], pieces, False
    )
    own_out, mate_out, partial = run(
        late_kernel,
        where,
        structure,
        [s2, s3, w_top, w_bottom, t1],
        [own_part, mate_part, own, s0, s1],
        pieces,
        True,
    )
    received = send(mate_out, Z_FLIP[1])

    quarter = width // 4
    cut = partial.reshape(2, 4, quarter, width)
    summed = lax.dynamic_index_in_dim(cut, y, 1, False)
    for d in (1, 2, 3):
        summed = summed + send(lax.dynamic_index_in_dim(cut, (y + d) & 3, 1, False), Y_BY[d])
    mine, mates = summed[0], summed[1]
    total = mine + send(mates, Z_FLIP[1]) + send(mine, Z_FLIP[2]) + send(mates, Z_FLIP[3])
    own_out, total = lax.optimization_barrier((own_out, total))
    diag = jnp.zeros((4, quarter, width), jnp.float32)
    diag = lax.dynamic_update_index_in_dim(diag, total, y, 0)
    for d in (1, 2, 3):
        diag = lax.dynamic_update_index_in_dim(diag, send(total, Y_BY[d]), (y - d) & 3, 0)
    return -(own_out + received), diag_inv + diag.reshape(1, width, width)


def solution(mesh):
    return jax.shard_map(
        local,
        mesh=mesh,
        in_specs=(P("pcol", None, "prow"), P("prow", "pcol"), P(), P("pcol", None, None)),
        out_specs=(P("pcol", "prow"), P("pcol", None, None)),
        check_vma=False,
    )
```

```python
import jax
import jax.numpy as jnp
from jax import lax
from jax.experimental import pallas as pl
from jax.experimental.pallas import tpu as pltpu
from jax.sharding import PartitionSpec as P


AXES = ("prow", "pcol")
TILE = 256


def number(x, y, z, core):
    return ((z >> 1) * 4 + y) * 16 + x * 4 + (z & 1) * 2 + core


def pairs(on=None, off=None):
    found = []
    for x in range(4):
        for y in range(4):
            for z in range(4):
                move = on if (y & 1) == (z & 1) else off
                if move is not None:
                    for core in range(2):
                        tx, ty, tz, tc = move(x, y, z, core)
                        found.append((number(x, y, z, core), number(tx % 4, ty % 4, tz % 4, tc)))
    return found


def shift(dy, dz):
    return lambda x, y, z, c: (x, y + dy, z + dz, c)


def both(move):
    return pairs(move, move)


X_UP = both(lambda x, y, z, c: (x + 1, y, z, c))
X_DOWN = both(lambda x, y, z, c: (x - 1, y, z, c))
CORE = both(lambda x, y, z, c: (x, y, z, 1 - c))
Y_BY = [None] + [both(shift(d, 0)) for d in (1, 2, 3)]
Z_FLIP = [None] + [both(lambda x, y, z, c, d=d: (x, y, z ^ d, c)) for d in (1, 2, 3)]


def send(array, route):
    return lax.ppermute(array, AXES, route)


def parts(value):
    high = value.astype(jnp.bfloat16)
    return high, (value - high.astype(jnp.float32)).astype(jnp.bfloat16)


def dot(a, b):
    return lax.dot_general(a, b, (((1,), (1,)), ((), ())), preferred_element_type=jnp.float32)


SLOTS = [
    ((0, -1), (-1, 2)),
    ((0, 1), (1, 2)),
    ((2, -1), (1, -1)),
    ((2, 1), (1, 1)),
    ((0, 0), (-1, 0)),
    ((2, 0), (1, 0)),
    ((0, 2), (-1, -1)),
    ((2, 2), (-1, 1)),
]


def slot_info(where, structure, entry, blocks):
    x, y, z, core = where[0], where[1], where[2], where[3]
    on = (y & 1) == (z & 1)
    ys = (y + jnp.where(on, entry[0][0], entry[1][0])) & 3
    zs = (z + jnp.where(on, entry[0][1], entry[1][1])) & 3
    block = (zs >> 1) * 4 + ys
    delta = ((block >> 1) - x) & 3
    place = jnp.where(delta == 0, 0, jnp.where(delta == 3, 1, delta + 1))
    supernode = x * 4 + (zs & 1) * 2 + core
    return place, (zs ^ z) & 1, [structure[supernode, block * blocks + b].astype(jnp.float32) for b in range(blocks)]


def multiply_kernel(where, structure, *refs):
    own, from_left, opposite, from_right, two_off, t0, w_top, w_bottom, t1, s0, s1, s2, s3, own_tile, s0_tile, s1_tile = refs[:16]
    pieces = refs[16:26]
    own_out, mate_top, mate_bottom, diag, high, low = refs[26:]
    rows, span = own.shape
    half = high.shape[2]
    blocks = span // rows
    step = pl.program_id(0)
    y, z, core = where[1], where[2], where[3]
    on = (y & 1) == (z & 1)

    @pl.when(step == 0)
    def _():
        def last(c):
            return jnp.where(on, jnp.concatenate([w_top[:, c], w_bottom[:, c]], axis=0), t1[:, c])

        def pick(a, b):
            return lambda c: jnp.where(on, a[:, c], b[:, c])

        values = [lambda c, ref=ref: ref[:, c] for ref in (s0, s1, s2, s3)]
        values += [pick(own, from_left), pick(opposite, from_right), pick(two_off, t0), last]
        for value, entry in zip(values, SLOTS):
            place, side, keeps = slot_info(where, structure, entry, blocks)
            row = pl.multiple_of(side * rows, rows)
            for b, keep in enumerate(keeps):
                hi, lo = parts(value(slice(b * rows, (b + 1) * rows)) * keep)
                g, inner = divmod(b * rows, half)
                at = place * 2 + (g ^ core)
                high[at, pl.ds(row, rows), inner : inner + rows] = hi
                low[at, pl.ds(row, rows), inner : inner + rows] = lo
        diag[...] = jnp.zeros(diag.shape, jnp.float32)

    first = step < pl.num_programs(0) // 2
    acc = jnp.zeros((2 * rows, TILE), jnp.float32)
    for j in range(8):
        if j < 6:
            value = pieces[j][...]
        else:
            value = jnp.where(first, pieces[2 * j - 6][...], pieces[2 * j - 5][...])
        a, b = parts(value)
        acc += dot(high[j], a) + dot(high[j], b) + dot(low[j], a)
    own_sum, mate_sum = acc[:rows], acc[rows:]
    own_out[...] = own_sum
    mate_top[...] = mate_sum[: rows // 2]
    mate_bottom[...] = mate_sum[rows // 2 :]

    column = ((z >> 1) * 4 + y) * blocks + step
    supernode = where[0] * 4 + (z & 1) * 2 + core
    keep_own = structure[supernode, column].astype(jnp.float32)
    keep_mate = structure[supernode ^ 2, column].astype(jnp.float32)
    panels = (own_tile[...] * keep_own, jnp.where((z & 1) == 1, s0_tile[...], s1_tile[...]) * keep_mate)
    for r, (result, panel) in enumerate(zip((own_sum, mate_sum), panels)):
        a, b = parts(result)
        c, d = parts(panel)
        diag[r] += dot(a, c) + dot(a, d) + dot(b, c)

    @pl.when(step == pl.num_programs(0) - 1)
    def _():
        total = diag[0]
        diag[0] = total + jnp.where(on, 0.0, total.T)
        diag[1] = jnp.where(on, diag[1], 0.0)


def multiply(where, structure, slots, tiles, pieces):
    rows, span = slots[0].shape
    half = span // 2
    middle = span // TILE // 2
    at_column = lambda height: pl.BlockSpec((height, TILE), lambda i, *_: (0, i))
    whole = lambda shape: pl.BlockSpec(shape, lambda i, *_: (0,) * len(shape))
    every = pl.BlockSpec((TILE, half), lambda i, *_: (i, 0))
    top = pl.BlockSpec((TILE, half), lambda i, *_: (jnp.minimum(i, middle - 1), 0))
    bottom = pl.BlockSpec((TILE, half), lambda i, *_: (jnp.maximum(i - middle, 0), 0))
    outs = [(rows, span), (rows // 2, span), (rows // 2, span), (2, rows, rows)]
    return pl.pallas_call(
        multiply_kernel,
        grid_spec=pltpu.PrefetchScalarGridSpec(
            num_scalar_prefetch=2,
            grid=(span // TILE,),
            in_specs=[whole(a.shape) for a in slots]
            + [at_column(rows)] * len(tiles)
            + [every] * 6
            + [top, bottom] * 2,
            out_specs=[at_column(shape[0]) for shape in outs[:3]] + [whole(outs[3])],
            scratch_shapes=[pltpu.VMEM((8, 2 * rows, half), jnp.bfloat16)] * 2,
        ),
        out_shape=[jax.ShapeDtypeStruct(shape, jnp.float32) for shape in outs],
        compiler_params=pltpu.CompilerParams(vmem_limit_bytes=60 * 2**20),
        cost_estimate=pl.CostEstimate(
            flops=48 * rows * span * span, bytes_accessed=4 * (rows * span * 16 + 4 * span * span), transcendentals=0
        ),
    )(where, structure, *slots, *tiles, *pieces)


def local(panel_t, ancestor, structure, diag_inv):
    width = panel_t.shape[1]
    span = panel_t.shape[2]
    prow = lax.axis_index("prow")
    pcol = lax.axis_index("pcol")
    x = pcol >> 2
    y = prow & 3
    z = (prow >> 2) * 2 + ((pcol >> 1) & 1)
    core = pcol & 1
    on = (y & 1) == (z & 1)
    own = panel_t.reshape(width, span)
    split = width // 2
    half = ancestor.shape[0] // 2

    from_left = send(own, both(shift(1, 0)))
    from_right = send(own, both(shift(-1, 0)))
    two_off = send(own, pairs(on=shift(0, 2)))
    opposite = jnp.concatenate(
        [send(from_left[:split], both(shift(1, 0))), send(from_right[split:], both(shift(-1, 0)))],
        axis=0,
    )
    turned = jnp.where(on, two_off, own)
    s0 = send(turned, pairs(on=shift(1, 0), off=shift(0, 1)))
    s1 = send(turned, pairs(on=shift(-1, 0), off=shift(0, -1)))
    t0 = send(from_left, pairs(on=shift(0, 1)))
    t1 = send(from_left, pairs(on=shift(0, -1)))
    crossed = jnp.where(on, from_right, opposite)
    s2 = send(crossed, pairs(on=shift(0, 1), off=shift(0, 1)))
    s3 = send(crossed, pairs(on=shift(0, -1), off=shift(0, -1)))
    w_top = send(s0[:split], pairs(off=shift(1, 0)))
    w_bottom = send(s1[split:], pairs(off=shift(-1, 0)))

    left = send(ancestor, X_UP)
    right = send(ancestor, X_DOWN)
    far = [send(left[:half], X_UP), send(right[half:], X_DOWN)]
    pieces = []
    for piece in (ancestor, left, right):
        pieces += [piece, send(piece, CORE)]
    pieces += far + [send(piece, CORE) for piece in far]

    where = jnp.stack([x, y, z, core]).astype(jnp.int32)
    slots = [own, from_left, opposite, from_right, two_off, t0, w_top, w_bottom, t1, s0, s1, s2, s3]
    own_out, mate_top, mate_bottom, partial = multiply(where, structure, slots, [own, s0, s1], pieces)
    received = jnp.concatenate([send(mate_top, Z_FLIP[1]), send(mate_bottom, Z_FLIP[1])], axis=0)

    quarter = width // 4
    cut = partial.reshape(2, 4, quarter, width)
    summed = lax.dynamic_index_in_dim(cut, y, 1, False)
    for d in (1, 2, 3):
        summed = summed + send(lax.dynamic_index_in_dim(cut, (y + d) & 3, 1, False), Y_BY[d])
    mine, mates = summed[0], summed[1]
    total = mine + send(mates, Z_FLIP[1]) + send(mine, Z_FLIP[2]) + send(mates, Z_FLIP[3])
    own_out, total = lax.optimization_barrier((own_out, total))
    diag = jnp.zeros((4, quarter, width), jnp.float32)
    diag = lax.dynamic_update_index_in_dim(diag, total, y, 0)
    for d in (1, 2, 3):
        diag = lax.dynamic_update_index_in_dim(diag, send(total, Y_BY[d]), (y - d) & 3, 0)
    return -(own_out + received), diag_inv + diag.reshape(1, width, width)


def solution(mesh):
    return jax.shard_map(
        local,
        mesh=mesh,
        in_specs=(P("pcol", None, "prow"), P("prow", "pcol"), P(), P("pcol", None, None)),
        out_specs=(P("pcol", "prow"), P("pcol", None, None)),
        check_vma=False,
    )
```

```python
import jax
import jax.numpy as jnp
from jax import lax
from jax.experimental import pallas as pl
from jax.experimental.pallas import tpu as pltpu
from jax.sharding import PartitionSpec as P


AXES = ("prow", "pcol")
TILE = 256


def number(x, y, z, core):
    return ((z >> 1) * 4 + y) * 16 + x * 4 + (z & 1) * 2 + core


def pairs(on=None, off=None):
    found = []
    for x in range(4):
        for y in range(4):
            for z in range(4):
                move = on if (y & 1) == (z & 1) else off
                if move is not None:
                    for core in range(2):
                        tx, ty, tz, tc = move(x, y, z, core)
                        found.append((number(x, y, z, core), number(tx % 4, ty % 4, tz % 4, tc)))
    return found


def shift(dy, dz):
    return lambda x, y, z, c: (x, y + (1 - 2 * c) * dy, z + (1 - 2 * c) * dz, c)


def both(move):
    return pairs(move, move)


X_UP = both(lambda x, y, z, c: (x + 1 - 2 * c, y, z, c))
X_DOWN = both(lambda x, y, z, c: (x - 1 + 2 * c, y, z, c))
CORE = both(lambda x, y, z, c: (x, y, z, 1 - c))
Y_BY = [None] + [both(shift(d, 0)) for d in (1, 2, 3)]
Z_FLIP = [None] + [both(lambda x, y, z, c, d=d: (x, y, z ^ d, c)) for d in (1, 2, 3)]


def send(array, route):
    return lax.ppermute(array, AXES, route)


def parts(value):
    high = value.astype(jnp.bfloat16)
    return high, (value - high.astype(jnp.float32)).astype(jnp.bfloat16)


def dot(a, b):
    return lax.dot_general(a, b, (((1,), (1,)), ((), ())), preferred_element_type=jnp.float32)


SLOTS = [
    ((0, -1), (-1, 2)),
    ((0, 1), (1, 2)),
    ((2, -1), (1, -1)),
    ((2, 1), (1, 1)),
    ((0, 0), (-1, 0)),
    ((2, 0), (1, 0)),
    ((0, 2), (-1, -1)),
    ((2, 2), (-1, 1)),
]


def slot_place(where, entry):
    x, y, z, core = where[0], where[1], where[2], where[3]
    on = (y & 1) == (z & 1)
    sign = 1 - 2 * core
    ys = (y + sign * jnp.where(on, entry[0][0], entry[1][0])) & 3
    zs = (z + sign * jnp.where(on, entry[0][1], entry[1][1])) & 3
    delta = (sign * ((((zs >> 1) * 4 + ys) >> 1) - x)) & 3
    place = jnp.where(delta == 0, 0, jnp.where(delta == 3, 1, delta + 1))
    return place * 2 + ((zs ^ z) & 1)


def multiply_kernel(where, structure, *refs):
    own, from_left, f_top, f_bottom, from_right, two_off, t0, w_top, w_bottom, t1, s0, s1, s2, s3 = refs[:14]
    pieces = refs[14:24]
    own_out, mate_top, mate_bottom, *cuts = refs[24:31]
    stage, high, low, result, panel, sems = refs[31:]
    rows, span = own.shape
    half = span // 2
    blocks = span // rows
    step = pl.program_id(0)
    x, y, z, core = where[0], where[1], where[2], where[3]
    on = (y & 1) == (z & 1)
    sign = 1 - 2 * core

    def copies(sources, at):
        height = rows // len(sources)
        for n, source in enumerate(sources):
            part = stage.at[at, pl.ds(n * height, height)]
            pltpu.make_async_copy(source, part, sems.at[at]).start()

    def arrived(at):
        pltpu.make_async_copy(stage.at[at], stage.at[at], sems.at[at]).wait()

    @pl.when(step == 0)
    def _():
        plain = [[ref] for ref in (s0, s1, s2, s3)]
        here = plain + [[own], [f_top, f_bottom], [two_off], [w_top, w_bottom]]
        there = plain + [[from_left], [from_right], [t0], [t1]]
        for a, b, entry in zip(here, there, SLOTS):
            at = slot_place(where, entry)
            if a is b:
                copies(a, at)
            else:
                pl.when(on)(lambda a=a, at=at: copies(a, at))
                pl.when(jnp.logical_not(on))(lambda b=b, at=at: copies(b, at))
        copies([own], 8)
        pl.when((z & 1) != core)(lambda: copies([s0], 9))
        pl.when((z & 1) == core)(lambda: copies([s1], 9))

    def cut_stage(j):
        block = ((x + sign * (0, -1, 1, 2)[j]) & 3) * 2 + (z & 1)
        for side in range(2):
            at = 2 * j + side
            arrived(at)
            supernode = x * 4 + ((z & 1) ^ side) * 2 + core
            for b in range(blocks):
                keep = structure[supernode, block * blocks + b].astype(jnp.float32)
                hi, lo = parts(stage[at, :, b * rows : (b + 1) * rows] * keep)
                g, inner = divmod(b * rows, half)
                row = slice(side * rows, (side + 1) * rows)
                high[2 * j + (g ^ core), row, inner : inner + rows] = hi
                low[2 * j + (g ^ core), row, inner : inner + rows] = lo

    first = step < pl.num_programs(0) // 2
    acc = jnp.zeros((2 * rows, TILE), jnp.float32)

    @pl.when(step == 0)
    def _():
        for j in range(4):
            cut_stage(j)

    for j in range(4):
        for k in range(2):
            if j < 3:
                value = pieces[2 * j + k][...]
            else:
                value = jnp.where(first, pieces[6 + 2 * k][...], pieces[7 + 2 * k][...])
            a, b = parts(value)
            acc += dot(high[2 * j + k], a) + dot(high[2 * j + k], b) + dot(low[2 * j + k], a)
    own_out[...] = acc[:rows]
    mate_top[...] = acc[rows : rows + mate_top.shape[0]]
    mate_bottom[...] = acc[rows + mate_top.shape[0] :]
    hi, lo = parts(acc)
    for side in range(2):
        result[step, side, :rows] = hi[side * rows : (side + 1) * rows]
        result[step, side, rows:] = lo[side * rows : (side + 1) * rows]

    @pl.when(step == 1)
    def _():
        block = (z >> 1) * 4 + y
        for side in range(2):
            arrived(8 + side)
            supernode = x * 4 + ((z & 1) ^ side) * 2 + core
            for b in range(blocks):
                c = slice(b * rows, (b + 1) * rows)
                keep = structure[supernode, block * blocks + b].astype(jnp.float32)
                panel[side, 0, :, c], panel[side, 1, :, c] = parts(stage[8 + side, :, c] * keep)

    @pl.when(step == pl.num_programs(0) - 1)
    def _():
        sums = []
        for side in range(2):
            sum_side = None
            for i in range(blocks):
                c = slice(i * rows, (i + 1) * rows)
                two = dot(result[i, side], panel[side, 0, :, c])
                term = two[:rows] + two[rows:] + dot(result[i, side, :rows], panel[side, 1, :, c])
                sum_side = term if sum_side is None else sum_side + term
            sums.append(sum_side)
        total = sums[0] + jnp.where(on, 0.0, sums[0].T)
        stage[0, :, :rows] = total
        stage[1, :, :rows] = jnp.where(on, sums[1], 0.0)
        quarter = rows // 4
        for d, ref in enumerate(cuts):
            at = pl.multiple_of(((y + sign * d) & 3) * quarter, quarter)
            for side in range(2):
                ref[side] = stage[side, pl.ds(at, quarter), :rows]


def multiply(where, structure, slots, pieces):
    rows, span = slots[0].shape
    half = span // 2
    middle = span // TILE // 2
    at_column = lambda height: pl.BlockSpec((height, TILE), lambda i, *_: (0, i))
    whole = lambda shape: pl.BlockSpec(shape, lambda i, *_: (0,) * len(shape))
    every = pl.BlockSpec((TILE, half), lambda i, *_: (i, 0))
    top = pl.BlockSpec((TILE, half), lambda i, *_: (jnp.minimum(i, middle - 1), 0))
    bottom = pl.BlockSpec((TILE, half), lambda i, *_: (jnp.maximum(i - middle, 0), 0))
    outs = [(rows, span), (rows * 5 // 8, span), (rows * 3 // 8, span)] + [(2, rows // 4, rows)] * 4
    return pl.pallas_call(
        multiply_kernel,
        grid_spec=pltpu.PrefetchScalarGridSpec(
            num_scalar_prefetch=2,
            grid=(span // TILE,),
            in_specs=[pl.BlockSpec(memory_space=pltpu.HBM)] * len(slots) + [every] * 6 + [top, bottom] * 2,
            out_specs=[at_column(shape[0]) for shape in outs[:3]] + [whole(shape) for shape in outs[3:]],
            scratch_shapes=[pltpu.VMEM((10, rows, span), jnp.float32)]
            + [pltpu.VMEM((8, 2 * rows, half), jnp.bfloat16)] * 2
            + [pltpu.VMEM((span // TILE, 2, 2 * rows, TILE), jnp.bfloat16)]
            + [pltpu.VMEM((2, 2, rows, span), jnp.bfloat16), pltpu.SemaphoreType.DMA((10,))],
        ),
        out_shape=[jax.ShapeDtypeStruct(shape, jnp.float32) for shape in outs],
        compiler_params=pltpu.CompilerParams(vmem_limit_bytes=56 * 2**20),
        cost_estimate=pl.CostEstimate(
            flops=48 * rows * span * span, bytes_accessed=4 * (rows * span * 16 + 4 * span * span), transcendentals=0
        ),
    )(where, structure, *slots, *pieces)


def local(panel_t, ancestor, structure, diag_inv):
    width = panel_t.shape[1]
    span = panel_t.shape[2]
    prow = lax.axis_index("prow")
    pcol = lax.axis_index("pcol")
    x = pcol >> 2
    y = prow & 3
    z = (prow >> 2) * 2 + ((pcol >> 1) & 1)
    core = pcol & 1
    on = (y & 1) == (z & 1)
    own = panel_t.reshape(width, span)
    split = width // 2
    half = ancestor.shape[0] // 2

    from_left = send(own, both(shift(1, 0)))
    from_right = send(own, both(shift(-1, 0)))
    two_off = send(own, pairs(on=shift(0, 2)))
    f_top = send(from_left[:split], both(shift(1, 0)))
    lower = from_right[split:]
    f_bottom = send(lower, both(shift(-1, 0)))
    turned = jnp.where(on, two_off, own)
    s0 = send(turned, pairs(on=shift(1, 0), off=shift(0, 1)))
    s1 = send(turned, pairs(on=shift(-1, 0), off=shift(0, -1)))
    t0 = send(from_left, pairs(on=shift(0, 1)))
    t1 = send(from_left, pairs(on=shift(0, -1)))
    crossed = jnp.where(on, from_right, jnp.concatenate([f_top, f_bottom], axis=0))
    s2 = send(crossed, pairs(on=shift(0, 1), off=shift(0, 1)))
    s3 = send(crossed, pairs(on=shift(0, -1), off=shift(0, -1)))
    w_top = send(s0[:split], pairs(off=shift(1, 0)))
    w_bottom = send(s1[split:], pairs(off=shift(-1, 0)))

    left = send(ancestor, X_UP)
    right = send(ancestor, X_DOWN)
    far = [send(left[:half], X_UP), send(right[half:], X_DOWN)]
    pieces = [ancestor, send(ancestor, CORE)]
    pieces += [left, send(right, CORE), right, send(left, CORE)]
    pieces += far + [send(piece, CORE) for piece in far]

    where = jnp.stack([x, y, z, core]).astype(jnp.int32)
    slots = [own, from_left, f_top, f_bottom, from_right, two_off, t0, w_top, w_bottom, t1, s0, s1, s2, s3]
    own_out, mate_top, mate_bottom, *cuts = multiply(where, structure, slots, pieces)
    received = jnp.concatenate([send(mate_top, Z_FLIP[1]), send(mate_bottom, Z_FLIP[1])], axis=0)

    quarter = width // 4
    summed = cuts[0]
    for d in (1, 2, 3):
        summed = summed + send(cuts[d], Y_BY[d])
    mine, mates = summed[0], summed[1]
    total = mine + send(mates, Z_FLIP[1]) + send(mine, Z_FLIP[2]) + send(mates, Z_FLIP[3])
    own_out, total = lax.optimization_barrier((own_out, total))
    diag = jnp.zeros((4, quarter, width), jnp.float32)
    diag = lax.dynamic_update_index_in_dim(diag, total, y, 0)
    for d in (1, 2, 3):
        diag = lax.dynamic_update_index_in_dim(diag, send(total, Y_BY[d]), (y - (1 - 2 * core) * d) & 3, 0)
    return -(own_out + received), diag_inv + diag.reshape(1, width, width)


def solution(mesh):
    return jax.shard_map(
        local,
        mesh=mesh,
        in_specs=(P("pcol", None, "prow"), P("prow", "pcol"), P(), P("pcol", None, None)),
        out_specs=(P("pcol", "prow"), P("pcol", None, None)),
        check_vma=False,
    )
```

```python
import jax
import jax.numpy as jnp
from jax import lax
from jax.experimental import pallas as pl
from jax.experimental.pallas import tpu as pltpu
from jax.sharding import PartitionSpec as P


AXES = ("prow", "pcol")
TILE = 256


def number(x, y, z, core):
    return ((z >> 1) * 4 + y) * 16 + x * 4 + (z & 1) * 2 + core


def pairs(on=None, off=None):
    found = []
    for x in range(4):
        for y in range(4):
            for z in range(4):
                move = on if (y & 1) == (z & 1) else off
                if move is not None:
                    for core in range(2):
                        tx, ty, tz, tc = move(x, y, z, core)
                        found.append((number(x, y, z, core), number(tx % 4, ty % 4, tz % 4, tc)))
    return found


def shift(dy, dz):
    return lambda x, y, z, c: (x, y + (1 - 2 * c) * dy, z + (1 - 2 * c) * dz, c)


def both(move):
    return pairs(move, move)


X_UP = both(lambda x, y, z, c: (x + 1 - 2 * c, y, z, c))
X_DOWN = both(lambda x, y, z, c: (x - 1 + 2 * c, y, z, c))
CORE = both(lambda x, y, z, c: (x, y, z, 1 - c))
Y_BY = [None] + [both(shift(d, 0)) for d in (1, 2, 3)]
Z_FLIP = [None] + [both(lambda x, y, z, c, d=d: (x, y, z ^ d, c)) for d in (1, 2, 3)]


def send(array, route):
    return lax.ppermute(array, AXES, route)


def parts(value):
    high = value.astype(jnp.bfloat16)
    return high, (value - high.astype(jnp.float32)).astype(jnp.bfloat16)


def dot(a, b):
    return lax.dot_general(a, b, (((1,), (1,)), ((), ())), preferred_element_type=jnp.float32)


SLOTS = [
    ((0, -1), (-1, 2)),
    ((0, 1), (1, 2)),
    ((2, -1), (1, -1)),
    ((2, 1), (1, 1)),
    ((0, 0), (-1, 0)),
    ((2, 0), (1, 0)),
    ((0, 2), (-1, -1)),
    ((2, 2), (-1, 1)),
]


def slot_place(where, entry):
    x, y, z, core = where[0], where[1], where[2], where[3]
    on = (y & 1) == (z & 1)
    sign = 1 - 2 * core
    ys = (y + sign * jnp.where(on, entry[0][0], entry[1][0])) & 3
    zs = (z + sign * jnp.where(on, entry[0][1], entry[1][1])) & 3
    delta = (sign * ((((zs >> 1) * 4 + ys) >> 1) - x)) & 3
    place = jnp.where(delta == 0, 0, jnp.where(delta == 3, 1, delta + 1))
    return place * 2 + ((zs ^ z) & 1)


def multiply_kernel(where, structure, *refs):
    own, from_left, f_top, f_bottom, from_right, two_off, t0, w_top, w_bottom, t1, s0, s1, s2, s3 = refs[:14]
    pieces = refs[14:24]
    own_out, mate_top, mate_bottom, *cuts = refs[24:31]
    stage, high, low, result, panel, sems = refs[31:]
    rows, span = own.shape
    half = span // 2
    blocks = span // rows
    step = pl.program_id(0)
    x, y, z, core = where[0], where[1], where[2], where[3]
    on = (y & 1) == (z & 1)
    sign = 1 - 2 * core

    def copies(sources, at):
        height = rows // len(sources)
        for n, source in enumerate(sources):
            part = stage.at[at, pl.ds(n * height, height)]
            pltpu.make_async_copy(source, part, sems.at[at]).start()

    def arrived(at):
        pltpu.make_async_copy(stage.at[at], stage.at[at], sems.at[at]).wait()

    @pl.when(step == 0)
    def _():
        plain = [[ref] for ref in (s0, s1, s2, s3)]
        here = plain + [[own], [f_top, f_bottom], [two_off], [w_top, w_bottom]]
        there = plain + [[from_left], [from_right], [t0], [t1]]
        for a, b, entry in zip(here, there, SLOTS):
            at = slot_place(where, entry)
            if a is b:
                copies(a, at)
            else:
                pl.when(on)(lambda a=a, at=at: copies(a, at))
                pl.when(jnp.logical_not(on))(lambda b=b, at=at: copies(b, at))
        copies([own], 8)
        pl.when((z & 1) != core)(lambda: copies([s0], 9))
        pl.when((z & 1) == core)(lambda: copies([s1], 9))

    def cut_stage(j):
        block = ((x + sign * (0, -1, 1, 2)[j]) & 3) * 2 + (z & 1)
        for side in range(2):
            at = 2 * j + side
            arrived(at)
            supernode = x * 4 + ((z & 1) ^ side) * 2 + core
            for b in range(blocks):
                keep = structure[supernode, block * blocks + b].astype(jnp.float32)
                hi, lo = parts(stage[at, :, b * rows : (b + 1) * rows] * keep)
                g, inner = divmod(b * rows, half)
                row = slice(side * rows, (side + 1) * rows)
                high[2 * j + (g ^ core), row, inner : inner + rows] = hi
                low[2 * j + (g ^ core), row, inner : inner + rows] = lo

    first = step < pl.num_programs(0) // 2
    acc = jnp.zeros((2 * rows, TILE), jnp.float32)

    @pl.when(step == 0)
    def _():
        for j in range(4):
            cut_stage(j)

    for j in range(4):
        for k in range(2):
            if j < 3:
                value = pieces[2 * j + k][...]
            else:
                value = jnp.where(first, pieces[6 + 2 * k][...], pieces[7 + 2 * k][...])
            a, b = parts(value)
            acc += dot(high[2 * j + k], a) + dot(high[2 * j + k], b) + dot(low[2 * j + k], a)
    own_out[...] = acc[:rows]
    mate_top[...] = acc[rows : rows + rows // 2]
    mate_bottom[...] = acc[rows + rows // 2 :]
    hi, lo = parts(acc)
    for side in range(2):
        result[step, side, :rows] = hi[side * rows : (side + 1) * rows]
        result[step, side, rows:] = lo[side * rows : (side + 1) * rows]

    @pl.when(step == 1)
    def _():
        block = (z >> 1) * 4 + y
        for side in range(2):
            arrived(8 + side)
            supernode = x * 4 + ((z & 1) ^ side) * 2 + core
            for b in range(blocks):
                c = slice(b * rows, (b + 1) * rows)
                keep = structure[supernode, block * blocks + b].astype(jnp.float32)
                panel[side, 0, :, c], panel[side, 1, :, c] = parts(stage[8 + side, :, c] * keep)

    @pl.when(step == pl.num_programs(0) - 1)
    def _():
        sums = []
        for side in range(2):
            sum_side = None
            for i in range(blocks):
                c = slice(i * rows, (i + 1) * rows)
                two = dot(result[i, side], panel[side, 0, :, c])
                term = two[:rows] + two[rows:] + dot(result[i, side, :rows], panel[side, 1, :, c])
                sum_side = term if sum_side is None else sum_side + term
            sums.append(sum_side)
        total = sums[0] + jnp.where(on, 0.0, sums[0].T)
        stage[0, :, :rows] = total
        stage[1, :, :rows] = jnp.where(on, sums[1], 0.0)
        quarter = rows // 4
        for d, ref in enumerate(cuts):
            at = pl.multiple_of(((y + sign * d) & 3) * quarter, quarter)
            for side in range(2):
                ref[side] = stage[side, pl.ds(at, quarter), :rows]


def multiply(where, structure, slots, pieces):
    rows, span = slots[0].shape
    half = span // 2
    middle = span // TILE // 2
    at_column = lambda height: pl.BlockSpec((height, TILE), lambda i, *_: (0, i))
    whole = lambda shape: pl.BlockSpec(shape, lambda i, *_: (0,) * len(shape))
    every = pl.BlockSpec((TILE, half), lambda i, *_: (i, 0))
    top = pl.BlockSpec((TILE, half), lambda i, *_: (jnp.minimum(i, middle - 1), 0))
    bottom = pl.BlockSpec((TILE, half), lambda i, *_: (jnp.maximum(i - middle, 0), 0))
    outs = [(rows, span), (rows // 2, span), (rows // 2, span)] + [(2, rows // 4, rows)] * 4
    return pl.pallas_call(
        multiply_kernel,
        grid_spec=pltpu.PrefetchScalarGridSpec(
            num_scalar_prefetch=2,
            grid=(span // TILE,),
            in_specs=[pl.BlockSpec(memory_space=pltpu.HBM)] * len(slots) + [every] * 6 + [top, bottom] * 2,
            out_specs=[at_column(shape[0]) for shape in outs[:3]] + [whole(shape) for shape in outs[3:]],
            scratch_shapes=[pltpu.VMEM((10, rows, span), jnp.float32)]
            + [pltpu.VMEM((8, 2 * rows, half), jnp.bfloat16)] * 2
            + [pltpu.VMEM((span // TILE, 2, 2 * rows, TILE), jnp.bfloat16)]
            + [pltpu.VMEM((2, 2, rows, span), jnp.bfloat16), pltpu.SemaphoreType.DMA((10,))],
        ),
        out_shape=[jax.ShapeDtypeStruct(shape, jnp.float32) for shape in outs],
        compiler_params=pltpu.CompilerParams(vmem_limit_bytes=56 * 2**20),
        cost_estimate=pl.CostEstimate(
            flops=48 * rows * span * span, bytes_accessed=4 * (rows * span * 16 + 4 * span * span), transcendentals=0
        ),
    )(where, structure, *slots, *pieces)


def local(panel_t, ancestor, structure, diag_inv):
    width = panel_t.shape[1]
    span = panel_t.shape[2]
    prow = lax.axis_index("prow")
    pcol = lax.axis_index("pcol")
    x = pcol >> 2
    y = prow & 3
    z = (prow >> 2) * 2 + ((pcol >> 1) & 1)
    core = pcol & 1
    on = (y & 1) == (z & 1)
    own = panel_t.reshape(width, span)
    split = width // 2
    half = ancestor.shape[0] // 2

    from_left = send(own, both(shift(1, 0)))
    from_right = send(own, both(shift(-1, 0)))
    two_off = send(own, pairs(on=shift(0, 2)))
    f_top = send(from_left[:split], both(shift(1, 0)))
    lower = from_right[split:]
    f_bottom = send(lower, both(shift(-1, 0)))
    turned = jnp.where(on, two_off, own)
    s0 = send(turned, pairs(on=shift(1, 0), off=shift(0, 1)))
    s1 = send(turned, pairs(on=shift(-1, 0), off=shift(0, -1)))
    t0 = send(from_left, pairs(on=shift(0, 1)))
    t1 = send(from_left, pairs(on=shift(0, -1)))
    crossed = jnp.where(on, from_right, jnp.concatenate([f_top, f_bottom], axis=0))
    s2 = send(crossed, pairs(on=shift(0, 1), off=shift(0, 1)))
    s3 = send(crossed, pairs(on=shift(0, -1), off=shift(0, -1)))
    w_top = send(s0[:split], pairs(off=shift(1, 0)))
    w_bottom = send(s1[split:], pairs(off=shift(-1, 0)))

    left = send(ancestor, X_UP)
    right = send(ancestor, X_DOWN)
    far = [send(left[:half], X_UP), send(right[half:], X_DOWN)]
    pieces = [ancestor, send(ancestor, CORE)]
    pieces += [left, send(right, CORE), right, send(left, CORE)]
    pieces += far + [send(piece, CORE) for piece in far]

    where = jnp.stack([x, y, z, core]).astype(jnp.int32)
    slots = [own, from_left, f_top, f_bottom, from_right, two_off, t0, w_top, w_bottom, t1, s0, s1, s2, s3]
    own_out, mate_top, mate_bottom, *cuts = multiply(where, structure, slots, pieces)
    received = jnp.concatenate([send(mate_top, Z_FLIP[1]), send(mate_bottom, Z_FLIP[1])], axis=0)

    quarter = width // 4
    summed = cuts[0]
    for d in (1, 2, 3):
        summed = summed + send(cuts[d], Y_BY[d])
    mine, mates = summed[0], summed[1]
    total = mine + send(mates, Z_FLIP[1]) + send(mine, Z_FLIP[2]) + send(mates, Z_FLIP[3])
    own_out, total = lax.optimization_barrier((own_out, total))
    diag = jnp.zeros((4, quarter, width), jnp.float32)
    diag = lax.dynamic_update_index_in_dim(diag, total, y, 0)
    for d in (1, 2, 3):
        diag = lax.dynamic_update_index_in_dim(diag, send(total, Y_BY[d]), (y - (1 - 2 * core) * d) & 3, 0)
    return -(own_out + received), diag_inv + diag.reshape(1, width, width)


def solution(mesh):
    return jax.shard_map(
        local,
        mesh=mesh,
        in_specs=(P("pcol", None, "prow"), P("prow", "pcol"), P(), P("pcol", None, None)),
        out_specs=(P("pcol", "prow"), P("pcol", None, None)),
        check_vma=False,
    )
```
